16 devices in a mesh: replica: 2 (over y, z), vocab: 8 (over x, core).
Axes of the slice: x: 4, y: 2, z: 1, core: 2. Of those that a mesh axis runs over, the one named last changes fastest.
The devices are a block of a 4x4x8 slice.
Arguments:
- hidden: bfloat16 [1024, 1536], P(('replica', 'vocab')), parts along dimension 0
- w_head: bfloat16 [151936, 1536], P('vocab')
- allowed_ids: int32 [1024, 64], P(('replica', 'vocab')), parts along dimension 0
- allowed_valid: int32 [1024, 64], P(('replica', 'vocab')), parts along dimension 0
- target_pos: int32 [1024], P(('replica', 'vocab')), parts along dimension 0
Outputs:
- output 1: float32 [1024, 64], P(('replica', 'vocab')), parts along dimension 0
- output 2: float32 [1024], P(('replica', 'vocab')), parts along dimension 0
There are 2 independent parts. The reference program is written for one: setup_inputs(seed, part) draws one part's arguments, and reference() takes and returns one part's arrays. A program takes and returns all parts, laid end to end along the dimension named above; an argument that names none is the same for every part.
All inputs are finite; a program needn't handle non-finite values.
Results may differ from the reference program's by a relative error of at most 0.001.
Values are sent between devices in bfloat16 or wider.
A program may use at most 768 MiB of HBM per device.

```python
import jax
import jax.numpy as jnp
from jax import lax

VOCAB_SIZE = 151936
MODEL_WIDTH = 1536
LIST_LEN = 64
ROWS_DEV = 64
GROUP_SIZE = 8
N_ROWS = GROUP_SIZE * ROWS_DEV
SHARD_LEN = VOCAB_SIZE // GROUP_SIZE
HOT_SLOTS = LIST_LEN // 2
WARM_SLOTS = LIST_LEN // 4
TEMPERATURE = 0.7


def draw_lists(key):
    k_perm, k_cold, k_tok, k_len, k_full, k_tgt = jax.random.split(key, 6)
    slot_pos = jnp.arange(LIST_LEN)
    category = jnp.where(slot_pos < HOT_SLOTS, 0, jnp.where(slot_pos < HOT_SLOTS + WARM_SLOTS, 1, 2))
    perm_keys = jax.random.split(k_perm, N_ROWS)
    slot_cat = jax.vmap(lambda k_row: jax.random.permutation(k_row, category))(perm_keys)
    cold_shard = jax.random.randint(k_cold, (N_ROWS, LIST_LEN), 2, GROUP_SIZE)
    shard_id = jnp.where(slot_cat == 2, cold_shard, slot_cat)
    offset = jax.random.randint(k_tok, (N_ROWS, LIST_LEN), 0, SHARD_LEN)
    allowed_ids = (shard_id * SHARD_LEN + offset).astype(jnp.int32)
    lengths = jax.random.randint(k_len, (N_ROWS,), 2, LIST_LEN + 1)
    full_row = jax.random.randint(k_full, (), 0, N_ROWS)
    lengths = jnp.where(jnp.arange(N_ROWS) == full_row, LIST_LEN, lengths)
    allowed_valid = (slot_pos[None, :] < lengths[:, None]).astype(jnp.int32)
    target_pos = jax.random.randint(k_tgt, (N_ROWS,), 0, lengths).astype(jnp.int32)
    return allowed_ids, allowed_valid, target_pos


def setup_inputs(seed: int = 0, part: int = 0) -> dict:
    base_key = jax.random.key(seed)
    shared_key, group_key = jax.random.split(base_key, 2)
    part_key = jax.random.fold_in(group_key, part)
    k_hidden, k_lists = jax.random.split(part_key, 2)
    hidden = jax.random.normal(k_hidden, (N_ROWS, MODEL_WIDTH), jnp.float32).astype(jnp.bfloat16)
    w_head = (jax.random.normal(shared_key, (VOCAB_SIZE, MODEL_WIDTH), jnp.float32) * MODEL_WIDTH ** -0.5).astype(jnp.bfloat16)
    allowed_ids, allowed_valid, target_pos = draw_lists(k_lists)
    return {"hidden": hidden, "w_head": w_head, "allowed_ids": allowed_ids, "allowed_valid": allowed_valid, "target_pos": target_pos}


def row_scores(hid_row, w_head, id_row):
    w_rows = jnp.take(w_head, id_row, axis=0)
    return jnp.dot(w_rows, hid_row, preferred_element_type=jnp.float32)


def reference(hidden, w_head, allowed_ids, allowed_valid, target_pos):
    raw_dots = lax.map(lambda row_pair: row_scores(row_pair[0], w_head, row_pair[1]), (hidden, allowed_ids))
    scores = raw_dots / TEMPERATURE
    valid_mask = allowed_valid > 0
    logits = jnp.where(valid_mask, scores, -jnp.inf)
    log_norm = jax.nn.logsumexp(logits, axis=1)
    allowed_prob = jnp.where(valid_mask, jnp.exp(logits - log_norm[:, None]), 0.0)
    picked = jnp.take_along_axis(scores, target_pos[:, None], axis=1)[:, 0]
    target_logp = picked - log_norm
    return allowed_prob, target_logp
```

```python
import functools

import jax
import jax.numpy as jnp
from jax import lax
from jax.experimental import pallas as pl
from jax.experimental.pallas import tpu as pltpu
from jax.sharding import PartitionSpec as P

TEMP = 0.7
LANES = 128
TILE = 1024
BLOCK = 256


def score_tile(h_ref, w_ref, s_ref, rows):
    for start in range(0, rows, BLOCK):
        width = min(BLOCK, rows - start)
        s_ref[:, start : start + width] = lax.dot_general(
            h_ref[...], w_ref[start : start + width, :], (((1,), (1,)), ((), ())), preferred_element_type=jnp.float32
        )


def pick_tile(s_ref, lane_ref, chunk_ref, out_ref, first_chunk, rows):
    for g in range(0, out_ref.shape[0], 8):
        lane = lane_ref[g : g + 8, :]
        rel = chunk_ref[g : g + 8, :] - first_chunk
        acc = out_ref[g : g + 8, :]
        for c in range(-(-rows // LANES)):
            x = s_ref[g : g + 8, c * LANES : (c + 1) * LANES]
            got = jnp.take_along_axis(x, lane, axis=1, mode="promise_in_bounds")
            acc = jnp.where(rel == c, got, acc)
        out_ref[g : g + 8, :] = acc


def scores_kernel(h_ref, lane_ref, chunk_ref, w_hbm, out_ref, w0, w1, s0, s1, sem):
    shard = w_hbm.shape[0]
    pairs = shard // (2 * TILE)
    tail = shard - pairs * 2 * TILE
    out_ref[...] = jnp.zeros_like(out_ref)

    def copy(tile, buf, k):
        return pltpu.make_async_copy(w_hbm.at[pl.ds(tile * TILE, TILE), :], buf, sem.at[k])

    def tail_copy(buf):
        return pltpu.make_async_copy(w_hbm.at[pl.ds(pairs * 2 * TILE, tail), :], buf.at[pl.ds(0, tail), :], sem.at[0])

    copy(0, w0, 0).start()
    copy(1, w1, 1).start()
    s1[...] = jnp.zeros_like(s1)

    def body(i, _):
        copy(2 * i, w0, 0).wait()
        score_tile(h_ref, w0, s0, TILE)
        pick_tile(s1, lane_ref, chunk_ref, out_ref, (2 * i - 1) * (TILE // LANES), TILE)

        @pl.when(i + 1 < pairs)
        def _():
            copy(2 * i + 2, w0, 0).start()

        @pl.when(i + 1 == pairs)
        def _():
            tail_copy(w0).start()

        copy(2 * i + 1, w1, 1).wait()
        score_tile(h_ref, w1, s1, TILE)
        pick_tile(s0, lane_ref, chunk_ref, out_ref, 2 * i * (TILE // LANES), TILE)

        @pl.when(i + 1 < pairs)
        def _():
            copy(2 * i + 3, w1, 1).start()

        return 0

    lax.fori_loop(0, pairs, body, 0)
    tail_copy(w0).wait()
    score_tile(h_ref, w0, s0, tail)
    pick_tile(s1, lane_ref, chunk_ref, out_ref, (2 * pairs - 1) * (TILE // LANES), TILE)
    pick_tile(s0, lane_ref, chunk_ref, out_ref, 2 * pairs * (TILE // LANES), tail)


def all_scores(h_all, lane, chunk, w_loc):
    n_rows, width = h_all.shape
    vmem = pl.BlockSpec(memory_space=pltpu.VMEM)
    return pl.pallas_call(
        scores_kernel,
        out_shape=jax.ShapeDtypeStruct((n_rows, LANES), jnp.float32),
        in_specs=[vmem, vmem, vmem, pl.BlockSpec(memory_space=pl.ANY)],
        out_specs=vmem,
        scratch_shapes=[
            pltpu.VMEM((TILE, width), jnp.bfloat16),
            pltpu.VMEM((TILE, width), jnp.bfloat16),
            pltpu.VMEM((n_rows, TILE), jnp.float32),
            pltpu.VMEM((n_rows, TILE), jnp.float32),
            pltpu.SemaphoreType.DMA((2,)),
        ],
        compiler_params=pltpu.CompilerParams(vmem_limit_bytes=40 * 1024 * 1024),
        name="scores",
    )(h_all, lane, chunk, w_loc)


def finish_rows(scores, valid_in, tgt_in):
    valid_mask = valid_in > 0
    logits = jnp.where(valid_mask, scores, -jnp.inf)
    log_norm = jax.nn.logsumexp(logits, axis=1)
    allowed_prob = jnp.where(valid_mask, jnp.exp(logits - log_norm[:, None]), 0.0)
    tgt_hit = tgt_in[:, None] == jnp.arange(scores.shape[1])[None, :]
    target_logp = jnp.sum(jnp.where(tgt_hit, scores, 0.0), axis=1) - log_norm
    return allowed_prob, target_logp


def solution(mesh):
    groups = mesh.shape["vocab"]
    rows_spec = P(("replica", "vocab"), None)
    vec_spec = P(("replica", "vocab"))

    def local_step(h_loc, w_loc, ids_loc, valid_loc, tgt_loc):
        n_rows, list_len = ids_loc.shape
        shard_len = w_loc.shape[0]
        me = lax.axis_index("vocab")
        half = h_loc.shape[1] // 2
        h_all = jnp.concatenate(
            [lax.all_gather(h_loc[:, :half], "vocab", tiled=True), lax.all_gather(h_loc[:, half:], "vocab", tiled=True)], axis=1
        )
        ids_all = lax.all_gather(ids_loc, "vocab", tiled=True)
        local = ids_all - me * shard_len
        mine = (local >= 0) & (local < shard_len)
        chunk = jnp.where(mine, local // LANES, -(2**20))
        lane = jnp.where(mine, local % LANES, 0)
        pad = ((0, 0), (0, LANES - list_len))
        part = all_scores(h_all, jnp.pad(lane, pad), jnp.pad(chunk, pad, constant_values=-(2**20)), w_loc)
        part = part[:, :list_len].reshape(groups, n_rows, list_len)
        back = lax.all_to_all(part, "vocab", 0, 0, tiled=True)
        scores = jnp.sum(back, axis=0) / TEMP
        return finish_rows(scores, valid_loc, tgt_loc)

    return jax.shard_map(
        local_step,
        mesh=mesh,
        in_specs=(rows_spec, P("vocab", None), rows_spec, rows_spec, vec_spec),
        out_specs=(rows_spec, vec_spec),
        check_vma=False,
    )
```

```python
import functools

import jax
import jax.numpy as jnp
from jax import lax
from jax.experimental import pallas as pl
from jax.experimental.pallas import tpu as pltpu
from jax.sharding import PartitionSpec as P

TEMP = 0.7
LANES = 128
TILE = 1024
BLOCK = 256
FAR = -(2**20)
PIECES = 16

SELF, PARTNER = 0, 2
LEFT_A, RIGHT_B = 4, 6
LEFT_B, RIGHT_A = 8, 10
ACROSS_A, ACROSS_B = 12, 14


def score_tile(h_ref, w_ref, s_ref, rows):
    for start in range(0, rows, BLOCK):
        width = min(BLOCK, rows - start)
        s_ref[:, start : start + width] = lax.dot_general(
            h_ref[...], w_ref[start : start + width, :], (((1,), (1,)), ((), ())), preferred_element_type=jnp.float32
        )


def pick_tile(s_ref, lane_ref, chunk_ref, out_ref, first_chunk, rows):
    low = lax.broadcasted_iota(jnp.int32, (8, LANES), 1) < LANES // 2
    for u in range(out_ref.shape[0] // 8):
        at = pl.ds(8 * u, 8)
        lane = lane_ref[at, :]
        rel = chunk_ref[at, :] - first_chunk
        acc = out_ref[at, :]
        for c in range(-(-rows // LANES)):
            cols = pl.ds(c * LANES, LANES)
            first = jnp.take_along_axis(s_ref[pl.ds(16 * u, 8), cols], lane, axis=1, mode="promise_in_bounds")
            second = jnp.take_along_axis(s_ref[pl.ds(16 * u + 8, 8), cols], lane, axis=1, mode="promise_in_bounds")
            acc = jnp.where(rel == c, jnp.where(low, first, second), acc)
        out_ref[at, :] = acc


def kernel(
    chips, h_ref, ids_ref, valid_ref, tgt_ref, w_hbm, p_ref, lp_ref,
    h_all, ids_all, chunk, lane, acc, back, w0, w1, s0, s1,
    w_sem, h_send, h_recv, i_send, i_recv, x_send, x_recv,
):
    n_rows, list_len = ids_ref.shape
    half = n_rows // 2
    packed = half // 2
    shard = w_hbm.shape[0]
    pairs = shard // (2 * TILE)
    tail = shard - pairs * 2 * TILE
    me = lax.axis_index("vocab")
    chip, core = me // 2, me % 2

    def place(hop, other):
        return {"vocab": lax.rem(chip + hop, chips) * 2 + (1 - core if other else core)}

    right, left, partner = place(1, False), place(chips - 1, False), place(0, True)

    def w_copy(tile, buf, k):
        return pltpu.make_async_copy(w_hbm.at[pl.ds(tile * TILE, TILE), :], buf, w_sem.at[k])

    def tail_copy(buf):
        return pltpu.make_async_copy(w_hbm.at[pl.ds(pairs * 2 * TILE, tail), :], buf.at[pl.ds(0, tail), :], w_sem.at[0])

    w_copy(0, w0, 0).start()
    w_copy(1, w1, 1).start()
    own = pltpu.make_async_copy(h_ref, h_all.at[pl.ds(0, n_rows), :], w_sem.at[2])
    own.start()
    barrier = pltpu.get_barrier_semaphore()
    for peer in (left, right, partner):
        pl.semaphore_signal(barrier, inc=1, device_id=peer, device_id_type=pl.DeviceIdType.MESH)

    listed = jnp.where(valid_ref[...] > 0, ids_ref[...], -1)
    for k in range(n_rows // 16):
        ids_all[pl.ds(8 * k, 8), :] = jnp.concatenate([listed[16 * k : 16 * k + 8], listed[16 * k + 8 : 16 * k + 16]], axis=1)
    acc[...] = jnp.zeros_like(acc)
    s1[...] = jnp.zeros_like(s1)
    pl.semaphore_wait(barrier, 3)

    sent = []

    def send(src, dst, count, peer):
        rows_h = h_ref.at[pl.ds(src * half, count * half), :] if src < PARTNER else h_all.at[pl.ds(src * half, half), :]
        copy_h = pltpu.make_async_remote_copy(
            src_ref=rows_h, dst_ref=h_all.at[pl.ds(dst * half, count * half), :],
            send_sem=h_send.at[len(sent)], recv_sem=h_recv.at[dst], device_id=peer, device_id_type=pl.DeviceIdType.MESH,
        )
        copy_i = pltpu.make_async_remote_copy(
            src_ref=ids_all.at[pl.ds(src * packed, count * packed), :], dst_ref=ids_all.at[pl.ds(dst * packed, count * packed), :],
            send_sem=i_send.at[len(sent)], recv_sem=i_recv.at[dst], device_id=peer, device_id_type=pl.DeviceIdType.MESH,
        )
        copy_h.start()
        copy_i.start()
        sent.append((copy_h, copy_i))

    def arrived(dst, count=1):
        pltpu.make_async_copy(h_all.at[pl.ds(dst * half, count * half), :], h_all.at[pl.ds(dst * half, count * half), :], h_recv.at[dst]).wait()
        pltpu.make_async_copy(ids_all.at[pl.ds(dst * packed, count * packed), :], ids_all.at[pl.ds(dst * packed, count * packed), :], i_recv.at[dst]).wait()

    send(0, LEFT_A, 1, right)
    send(1, RIGHT_B, 1, left)
    send(0, PARTNER, 2, partner)
    send(1, LEFT_B, 1, right)
    send(0, RIGHT_A, 1, left)
    arrived(LEFT_A)
    send(LEFT_A, ACROSS_A, 1, right)
    send(LEFT_A, LEFT_A + 1, 1, partner)
    arrived(RIGHT_B)
    send(RIGHT_B, ACROSS_B, 1, left)
    send(RIGHT_B, RIGHT_B + 1, 1, partner)
    for piece in (LEFT_B, RIGHT_A, ACROSS_A, ACROSS_B):
        arrived(piece)
        send(piece, piece + 1, 1, partner)
    arrived(PARTNER, 2)
    for piece in (LEFT_A, RIGHT_B, LEFT_B, RIGHT_A, ACROSS_A, ACROSS_B):
        arrived(piece + 1)
    own.wait()

    for u in range(PIECES * packed // 8):
        at = pl.ds(8 * u, 8)
        local = ids_all[at, :] - me * shard
        mine = (local >= 0) & (local < shard)
        chunk[at, :] = jnp.where(mine, lax.shift_right_arithmetic(local, 7), FAR)
        lane[at, :] = local & (LANES - 1)

    def body(i, _):
        w_copy(2 * i, w0, 0).wait()
        score_tile(h_all, w0, s0, TILE)
        pick_tile(s1, lane, chunk, acc, (2 * i - 1) * (TILE // LANES), TILE)

        @pl.when(i + 1 < pairs)
        def _():
            w_copy(2 * i + 2, w0, 0).start()

        @pl.when(i + 1 == pairs)
        def _():
            tail_copy(w0).start()

        w_copy(2 * i + 1, w1, 1).wait()
        score_tile(h_all, w1, s1, TILE)
        pick_tile(s0, lane, chunk, acc, 2 * i * (TILE // LANES), TILE)

        @pl.when(i + 1 < pairs)
        def _():
            w_copy(2 * i + 3, w1, 1).start()

        return 0

    lax.fori_loop(0, pairs, body, 0)
    tail_copy(w0).wait()
    score_tile(h_all, w0, s0, tail)
    pick_tile(s1, lane, chunk, acc, (2 * pairs - 1) * (TILE // LANES), TILE)
    pick_tile(s0, lane, chunk, acc, 2 * pairs * (TILE // LANES), tail)

    exits = []
    for hop, first, second in ((2, ACROSS_A, ACROSS_B), (chips - 1, LEFT_A, LEFT_B), (1, RIGHT_A, RIGHT_B), (0, PARTNER, PARTNER + 1)):
        for other in (False, True):
            if hop == 0 and not other:
                continue
            slot = ((chips - hop) % chips) * 2 + int(other)
            for part, piece in enumerate((first, second)):
                shift = int(other) if hop else 0
                out = pltpu.make_async_remote_copy(
                    src_ref=acc.at[pl.ds((piece + shift) * packed, packed), :],
                    dst_ref=back.at[slot, pl.ds(part * packed, packed), :],
                    send_sem=x_send.at[2 * slot + part], recv_sem=x_recv.at[2 * slot + part],
                    device_id=place(hop, other), device_id_type=pl.DeviceIdType.MESH,
                )
                out.start()
                exits.append(out)
    total = acc[pl.ds(0, 2 * packed), :]
    for out in exits:
        out.wait()
    for slot in range(1, 2 * chips):
        total = total + back[slot]

    rows = []
    for k in range(n_rows // 16):
        rows += [total[8 * k : 8 * k + 8, :list_len], total[8 * k : 8 * k + 8, list_len:]]
    scores = jnp.concatenate(rows, axis=0) / TEMP
    keep = valid_ref[...] > 0
    logits = jnp.where(keep, scores, -jnp.inf)
    top = jnp.max(logits, axis=1, keepdims=True)
    log_norm = top + jnp.log(jnp.sum(jnp.exp(logits - top), axis=1, keepdims=True))
    p_ref[...] = jnp.where(keep, jnp.exp(logits - log_norm), 0.0)
    row_id = lax.broadcasted_iota(jnp.int32, (n_rows, n_rows), 0)
    col_id = lax.broadcasted_iota(jnp.int32, (n_rows, n_rows), 1)
    eye = row_id == col_id
    target = jnp.sum(jnp.where(eye, jnp.broadcast_to(tgt_ref[...].astype(jnp.float32), (n_rows, n_rows)), 0.0), axis=1, keepdims=True)
    place_id = lax.broadcasted_iota(jnp.int32, (n_rows, list_len), 1).astype(jnp.float32)
    picked = jnp.sum(jnp.where(place_id == target, scores, 0.0), axis=1, keepdims=True)
    lp = picked - log_norm
    lp_ref[...] = jnp.sum(jnp.where(eye, jnp.broadcast_to(lp, (n_rows, n_rows)), 0.0), axis=0, keepdims=True)
    for copy_h, copy_i in sent:
        copy_h.wait_send()
        copy_i.wait_send()


def solution(mesh):
    groups = mesh.shape["vocab"]
    rows_spec = P(("replica", "vocab"), None)
    vec_spec = P(("replica", "vocab"))

    def local_step(h_loc, w_loc, ids_loc, valid_loc, tgt_loc):
        n_rows, list_len = ids_loc.shape
        width = h_loc.shape[1]
        all_rows = groups * n_rows
        vmem = pl.BlockSpec(memory_space=pltpu.VMEM)
        n_sent = 13
        p, lp = pl.pallas_call(
            functools.partial(kernel, groups // 2),
            out_shape=(jax.ShapeDtypeStruct((n_rows, list_len), jnp.float32), jax.ShapeDtypeStruct((1, n_rows), jnp.float32)),
            in_specs=[vmem, vmem, vmem, vmem, pl.BlockSpec(memory_space=pl.ANY)],
            out_specs=(vmem, vmem),
            scratch_shapes=[
                pltpu.VMEM((all_rows, width), jnp.bfloat16),
                pltpu.VMEM((all_rows // 2, LANES), jnp.int32),
                pltpu.VMEM((all_rows // 2, LANES), jnp.int32),
                pltpu.VMEM((all_rows // 2, LANES), jnp.int32),
                pltpu.VMEM((all_rows // 2, LANES), jnp.float32),
                pltpu.VMEM((groups, n_rows // 2, LANES), jnp.float32),
                pltpu.VMEM((TILE, width), jnp.bfloat16),
                pltpu.VMEM((TILE, width), jnp.bfloat16),
                pltpu.VMEM((all_rows, TILE), jnp.float32),
                pltpu.VMEM((all_rows, TILE), jnp.float32),
                pltpu.SemaphoreType.DMA((3,)),
                pltpu.SemaphoreType.DMA((n_sent,)),
                pltpu.SemaphoreType.DMA((PIECES,)),
                pltpu.SemaphoreType.DMA((n_sent,)),
                pltpu.SemaphoreType.DMA((PIECES,)),
                pltpu.SemaphoreType.DMA((2 * groups,)),
                pltpu.SemaphoreType.DMA((2 * groups,)),
            ],
            compiler_params=pltpu.CompilerParams(vmem_limit_bytes=48 * 1024 * 1024, collective_id=0, has_side_effects=True),
            name="fused",
        )(h_loc, ids_loc, valid_loc, tgt_loc.reshape(1, n_rows), w_loc)
        return p, lp.reshape(n_rows)

    return jax.shard_map(
        local_step,
        mesh=mesh,
        in_specs=(rows_spec, P("vocab", None), rows_spec, rows_spec, vec_spec),
        out_specs=(rows_spec, vec_spec),
        check_vma=False,
    )
```

```python
import functools

import jax
import jax.numpy as jnp
from jax import lax
from jax.experimental import pallas as pl
from jax.experimental.pallas import tpu as pltpu
from jax.sharding import PartitionSpec as P

TEMP = 0.7
LANES = 128
TILE = 1024
BLOCK = 256
CHUNKS = TILE // LANES
FAR = -(2**20)
NEVER = 2**21
PIECES = 16
SLOTS = 12
EARLY_CHIP = 4
EARLY_HALF = 6
AHEAD = 3
MESH = pl.DeviceIdType.MESH

PARTNER = 2
LEFT_A, RIGHT_B = 4, 6
LEFT_B, RIGHT_A = 8, 10
ACROSS_A, ACROSS_B = 12, 14


def score_tile(h_ref, w_ref, slot, s_ref, lo, hi, rows):
    for start in range(0, rows, BLOCK):
        width = min(BLOCK, rows - start)
        s_ref[lo:hi, start : start + width] = lax.dot_general(
            h_ref[lo:hi, :], w_ref[slot, start : start + width, :], (((1,), (1,)), ((), ())), preferred_element_type=jnp.float32
        )


def permute(x, lane):
    dims = lax.GatherDimensionNumbers(
        offset_dims=(), collapsed_slice_dims=(1,), start_index_map=(1,), operand_batching_dims=(0,), start_indices_batching_dims=(0,)
    )
    return lax.gather(x, lane[:, :, None], dims, (1, 1), mode=lax.GatherScatterMode.PROMISE_IN_BOUNDS)


def pick_tile(s_ref, lane_ref, chunk_ref, out_ref, lo, hi, first_chunk, rows):
    low = lax.broadcasted_iota(jnp.int32, (8, LANES), 1) < LANES // 2
    for u in range(lo // 16, hi // 16):
        at = pl.ds(8 * u, 8)
        row = 32 * (u // 2) + 8 * (u % 2)
        lane = lane_ref[at, :]
        rel = chunk_ref[at, :] - first_chunk
        acc = out_ref[at, :]
        for c in range(-(-rows // LANES)):
            cols = pl.ds(c * LANES, LANES)
            first = permute(s_ref[pl.ds(row, 8), cols], lane)
            second = permute(s_ref[pl.ds(row + 16, 8), cols], lane)
            acc = jnp.where(rel == c, jnp.where(low, first, second), acc)
        out_ref[at, :] = acc


def kernel(
    chips, h_hbm, ids_hbm, valid_hbm, tgt_hbm, w_hbm, p_ref, lp_ref,
    h_all, ids_in, valid_in, tgt_in, ids_all, chunk, lane, acc, back, wbuf, s0, s1,
    in_sem, w_sem, h_send, h_recv, i_send, i_recv, x_send, x_recv,
):
    n_rows, list_len = ids_in.shape
    half = n_rows // 2
    packed = half // 2
    all_rows = h_all.shape[0]
    shard = w_hbm.shape[0]
    full = shard // TILE
    tail = shard - full * TILE
    me = lax.axis_index("vocab")
    chip, core = me // 2, me % 2

    def place(hop, other):
        return {"vocab": lax.rem(chip + hop, chips) * 2 + (1 - core if other else core)}

    right, left, partner = place(1, False), place(chips - 1, False), place(0, True)

    def w_copy(tile):
        slot = lax.rem(tile, SLOTS)
        return pltpu.make_async_copy(w_hbm.at[pl.ds(tile * TILE, TILE), :], wbuf.at[slot], w_sem.at[slot])

    def tail_copy():
        slot = full % SLOTS
        return pltpu.make_async_copy(w_hbm.at[pl.ds(full * TILE, tail), :], wbuf.at[slot, pl.ds(0, tail), :], w_sem.at[slot])

    inputs = [
        pltpu.make_async_copy(h_hbm, h_all.at[pl.ds(0, n_rows), :], in_sem.at[0]),
        pltpu.make_async_copy(ids_hbm, ids_in, in_sem.at[1]),
        pltpu.make_async_copy(valid_hbm, valid_in, in_sem.at[2]),
        pltpu.make_async_copy(tgt_hbm, tgt_in, in_sem.at[3]),
    ]
    for copy in inputs:
        copy.start()
    for t in range(AHEAD):
        w_copy(t).start()
    barrier = pltpu.get_barrier_semaphore()
    for peer in (left, right, partner):
        pl.semaphore_signal(barrier, inc=1, device_id=peer, device_id_type=MESH)
    acc[...] = jnp.zeros_like(acc)
    s1[...] = jnp.zeros_like(s1)
    inputs[1].wait()
    inputs[2].wait()
    listed = jnp.where(valid_in[...] > 0, ids_in[...], -1)
    for k in range(2):
        ids_all[pl.ds(packed * k, packed), :] = jnp.concatenate(
            [listed[half * k : half * k + packed], listed[half * k + packed : half * (k + 1)]], axis=1
        )
    pl.semaphore_wait(barrier, 3)
    inputs[0].wait()

    def hop(k, src, dst, count, peer):
        return (
            pltpu.make_async_remote_copy(
                src_ref=h_all.at[pl.ds(src * half, count * half), :], dst_ref=h_all.at[pl.ds(dst * half, count * half), :],
                send_sem=h_send.at[k], recv_sem=h_recv.at[dst], device_id=peer, device_id_type=MESH,
            ),
            pltpu.make_async_remote_copy(
                src_ref=ids_all.at[pl.ds(src * packed, count * packed), :], dst_ref=ids_all.at[pl.ds(dst * packed, count * packed), :],
                send_sem=i_send.at[k], recv_sem=i_recv.at[dst], device_id=peer, device_id_type=MESH,
            ),
        )

    sent = []

    def send(*moves):
        started = []
        for move in moves:
            args = (len(sent), *move)
            sent.append(args)
            started.append(hop(*args))
        for which in range(2):
            for pair in started:
                pair[which].start()

    def arrived(dst, count=1):
        for ref, size, sem in ((h_all, half, h_recv), (ids_all, packed, i_recv)):
            there = ref.at[pl.ds(dst * size, count * size), :]
            pltpu.make_async_copy(there, there, sem.at[dst]).wait()

    def prepare(first, last):
        at = pl.ds(first * packed, (last - first) * packed)
        local = ids_all[at, :] - me * shard
        mine = (local >= 0) & (local < shard)
        chunk[at, :] = jnp.where(mine, lax.shift_right_arithmetic(local, 7), FAR)
        lane[at, :] = local & (LANES - 1)

    def neighbours_first():
        arrived(LEFT_A)
        send((LEFT_A, ACROSS_A, 1, right), (LEFT_A, LEFT_A + 1, 1, partner))
        arrived(RIGHT_B)
        send((RIGHT_B, ACROSS_B, 1, left), (RIGHT_B, RIGHT_B + 1, 1, partner))

    def pass_on(*pieces):
        for piece in pieces:
            arrived(piece)
            send((piece, piece + 1, 1, partner))

    def phase(first, count, lo, hi, wait=True, ahead=False, refill=False, events={}):
        def body(i, _):
            t = first + 2 * i
            for when, event in events.items():
                pl.when(i == when)(event)
            if wait:
                w_copy(t).wait()
            if ahead:
                for k in range(2):
                    pl.when(t + AHEAD + k < SLOTS)(w_copy(t + AHEAD + k).start)
            score_tile(h_all, wbuf, lax.rem(t, SLOTS), s0, lo, hi, TILE)
            pick_tile(s1, lane, chunk, acc, lo, hi, jnp.where(i > 0, (t - 1) * CHUNKS, NEVER), TILE)
            if wait:
                w_copy(t + 1).wait()
            score_tile(h_all, wbuf, lax.rem(t + 1, SLOTS), s1, lo, hi, TILE)
            pick_tile(s0, lane, chunk, acc, lo, hi, t * CHUNKS, TILE)
            if refill:
                for k in range(2):
                    pl.when(t + k + SLOTS < full)(w_copy(t + k + SLOTS).start)
                    pl.when(t + k + SLOTS == full)(tail_copy().start)
            return 0

        lax.fori_loop(0, count // 2, body, 0)

    def last_pick(tile, lo, hi):
        pick_tile(s1, lane, chunk, acc, lo, hi, tile * CHUNKS, TILE)

    early = EARLY_CHIP + EARLY_HALF
    send((0, LEFT_A, 1, right), (1, RIGHT_B, 1, left), (0, PARTNER, 2, partner), (1, LEFT_B, 1, right), (0, RIGHT_A, 1, left))
    prepare(0, 2)
    arrived(PARTNER, 2)
    prepare(PARTNER, PARTNER + 2)
    phase(0, EARLY_CHIP, 0, all_rows // 4, ahead=True, events={1: neighbours_first})
    last_pick(EARLY_CHIP - 1, 0, all_rows // 4)
    arrived(LEFT_A + 1)
    arrived(RIGHT_B + 1)
    prepare(LEFT_A, RIGHT_B + 2)
    phase(
        EARLY_CHIP, EARLY_HALF, 0, all_rows // 2, ahead=True,
        events={1: lambda: pass_on(LEFT_B, RIGHT_A), 2: lambda: pass_on(ACROSS_A, ACROSS_B)},
    )
    last_pick(early - 1, 0, all_rows // 2)
    for piece in (LEFT_B, RIGHT_A, ACROSS_A, ACROSS_B):
        arrived(piece + 1)
    prepare(LEFT_B, PIECES)
    phase(0, EARLY_CHIP, all_rows // 4, all_rows, wait=False, refill=True)
    last_pick(EARLY_CHIP - 1, all_rows // 4, all_rows)
    phase(EARLY_CHIP, EARLY_HALF, all_rows // 2, all_rows, wait=False, refill=True)
    last_pick(early - 1, all_rows // 2, all_rows)
    phase(early, full - early, 0, all_rows)
    tail_copy().wait()
    score_tile(h_all, wbuf, full % SLOTS, s0, 0, all_rows, tail)
    last_pick(full - 1, 0, all_rows)
    pick_tile(s0, lane, chunk, acc, 0, all_rows, full * CHUNKS, tail)

    exits = []
    for hops, first, second in ((2, ACROSS_A, ACROSS_B), (chips - 1, LEFT_A, LEFT_B), (1, RIGHT_A, RIGHT_B), (0, PARTNER, PARTNER + 1)):
        for other in (False, True):
            if hops == 0 and not other:
                continue
            slot = ((chips - hops) % chips) * 2 + int(other)
            for part, piece in enumerate((first, second)):
                shift = int(other) if hops else 0
                out = pltpu.make_async_remote_copy(
                    src_ref=acc.at[pl.ds((piece + shift) * packed, packed), :],
                    dst_ref=back.at[slot, pl.ds(part * packed, packed), :],
                    send_sem=x_send.at[2 * slot + part], recv_sem=x_recv.at[2 * slot + part],
                    device_id=place(hops, other), device_id_type=MESH,
                )
                out.start()
                exits.append(out)
    inputs[3].wait()
    keep = valid_in[...] > 0
    row_id = lax.broadcasted_iota(jnp.int32, (n_rows, n_rows), 0)
    col_id = lax.broadcasted_iota(jnp.int32, (n_rows, n_rows), 1)
    eye = row_id == col_id
    target = jnp.sum(jnp.where(eye, jnp.broadcast_to(tgt_in[...].astype(jnp.float32), (n_rows, n_rows)), 0.0), axis=1, keepdims=True)
    total = acc[pl.ds(0, 2 * packed), :]
    for args in sent:
        for copy in hop(*args):
            copy.wait_send()
    for out in exits:
        out.wait()
    for slot in range(1, 2 * chips):
        total = total + back[slot]

    rows = []
    for k in range(2):
        rows += [total[packed * k : packed * (k + 1), :list_len], total[packed * k : packed * (k + 1), list_len:]]
    scores = jnp.concatenate(rows, axis=0) / TEMP
    logits = jnp.where(keep, scores, -jnp.inf)
    top = jnp.max(logits, axis=1, keepdims=True)
    log_norm = top + jnp.log(jnp.sum(jnp.exp(logits - top), axis=1, keepdims=True))
    p_ref[...] = jnp.where(keep, jnp.exp(logits - log_norm), 0.0)
    place_id = lax.broadcasted_iota(jnp.int32, (n_rows, list_len), 1).astype(jnp.float32)
    picked = jnp.sum(jnp.where(place_id == target, scores, 0.0), axis=1, keepdims=True)
    lp = picked - log_norm
    lp_ref[...] = jnp.sum(jnp.where(eye, jnp.broadcast_to(lp, (n_rows, n_rows)), 0.0), axis=0, keepdims=True)


def solution(mesh):
    groups = mesh.shape["vocab"]
    rows_spec = P(("replica", "vocab"), None)
    vec_spec = P(("replica", "vocab"))

    def local_step(h_loc, w_loc, ids_loc, valid_loc, tgt_loc):
        n_rows, list_len = ids_loc.shape
        width = h_loc.shape[1]
        all_rows = groups * n_rows
        vmem = pl.BlockSpec(memory_space=pltpu.VMEM)
        hbm = pl.BlockSpec(memory_space=pltpu.HBM)
        lists = pltpu.VMEM((all_rows // 2, LANES), jnp.int32)
        scores = pltpu.VMEM((all_rows, TILE), jnp.float32)
        sems = pltpu.SemaphoreType.DMA
        p, lp = pl.pallas_call(
            functools.partial(kernel, groups // 2),
            out_shape=(jax.ShapeDtypeStruct((n_rows, list_len), jnp.float32), jax.ShapeDtypeStruct((1, n_rows), jnp.float32)),
            in_specs=[hbm] * 5,
            out_specs=(vmem, vmem),
            scratch_shapes=[
                pltpu.VMEM((all_rows, width), jnp.bfloat16),
                pltpu.VMEM((n_rows, list_len), jnp.int32),
                pltpu.VMEM((n_rows, list_len), jnp.int32),
                pltpu.VMEM((1, n_rows), jnp.int32),
                lists, lists, lists,
                pltpu.VMEM((all_rows // 2, LANES), jnp.float32),
                pltpu.VMEM((groups, n_rows // 2, LANES), jnp.float32),
                pltpu.VMEM((SLOTS, TILE, width), jnp.bfloat16),
                scores, scores,
                sems((4,)), sems((SLOTS,)), sems((PIECES,)), sems((PIECES,)), sems((PIECES,)), sems((PIECES,)),
                sems((2 * groups,)), sems((2 * groups,)),
            ],
            compiler_params=pltpu.CompilerParams(vmem_limit_bytes=56 * 1024 * 1024, collective_id=0, has_side_effects=True),
            name="fused",
        )(h_loc, ids_loc, valid_loc, tgt_loc.reshape(1, n_rows), w_loc)
        return p, lp.reshape(n_rows)

    return jax.shard_map(
        local_step,
        mesh=mesh,
        in_specs=(rows_spec, P("vocab", None), rows_spec, rows_spec, vec_spec),
        out_specs=(rows_spec, vec_spec),
        check_vma=False,
    )
```
